32 devices in a mesh: ep: 32 (over z, y, x, core).
Axes of the slice: x: 2, y: 2, z: 4, core: 2. Of those that a mesh axis runs over, the one named last changes fastest.
Arguments:
- x_tokens: bfloat16 [32768, 1024], P('ep')
- w_router: bfloat16 [1024, 32], replicated
- w_gate: bfloat16 [32, 1024, 512], P('ep')
- w_up: bfloat16 [32, 1024, 512], P('ep')
- w_down: bfloat16 [32, 512, 1024], P('ep')
- topk_idx: int32 [32768, 8], P('ep')
- dy_tokens: bfloat16 [32768, 1024], P('ep')
Outputs:
- output 1: bfloat16 [32768, 1024], P('ep')
- output 2: float32 [], replicated
- output 3: bfloat16 [32768, 1024], P('ep')
- output 4: float32 [1024, 32], replicated
- output 5: float32 [32, 1024, 512], P('ep')
- output 6: float32 [32, 1024, 512], P('ep')
- output 7: float32 [32, 512, 1024], P('ep')
All inputs are finite; a program needn't handle non-finite values.
Results may differ from the reference program's by a relative error of at most 0.00541992.
Values are sent between devices in bfloat16 or wider.
A program may use at most 1 GiB of HBM per device.

```python
import jax
import jax.numpy as jnp
from jax import lax

MODEL_DIM = 1024
FF_DIM = 512
NUM_EXPERTS = 32
TOP_K = 8
TOK_PER_DEV = 1024
NUM_DEVICES = 32
ALL_TOKENS = NUM_DEVICES * TOK_PER_DEV
CAPACITY = (5 * TOK_PER_DEV * TOP_K + 4 * NUM_EXPERTS - 1) // (4 * NUM_EXPERTS)
AUX_COEF = 0.001


def draw_routing(key):
    bias_key, score_key = jax.random.split(key)
    dev_bias = jax.random.randint(bias_key, (NUM_DEVICES, 1, NUM_EXPERTS), 0, 61)
    scores = jax.random.randint(score_key, (NUM_DEVICES, TOK_PER_DEV, NUM_EXPERTS), 0, 1000)
    ranked = (scores + dev_bias) * NUM_EXPERTS + jnp.arange(NUM_EXPERTS, dtype=jnp.int32)
    chosen = lax.top_k(ranked, TOP_K)[1]
    return chosen.reshape(ALL_TOKENS, TOP_K).astype(jnp.int32)


def setup_inputs(seed: int = 0) -> dict:
    key_list = jax.random.split(jax.random.key(seed), 7)
    topk_idx = draw_routing(key_list[0])
    router_f = jax.random.normal(key_list[1], (MODEL_DIM, NUM_EXPERTS), jnp.float32) * MODEL_DIM ** -0.5
    chosen_hot = jnp.zeros((ALL_TOKENS, NUM_EXPERTS), jnp.float32).at[jnp.arange(ALL_TOKENS)[:, None], topk_idx].set(1.0)
    x_noise = jax.random.normal(key_list[2], (ALL_TOKENS, MODEL_DIM), jnp.float32)
    x_tokens = x_noise + 3.0 * jnp.dot(chosen_hot, router_f.T)
    w_gate = jax.random.normal(key_list[3], (NUM_EXPERTS, MODEL_DIM, FF_DIM), jnp.float32) * MODEL_DIM ** -0.5
    w_up = jax.random.normal(key_list[4], (NUM_EXPERTS, MODEL_DIM, FF_DIM), jnp.float32) * MODEL_DIM ** -0.5
    w_down = jax.random.normal(key_list[5], (NUM_EXPERTS, FF_DIM, MODEL_DIM), jnp.float32) * FF_DIM ** -0.5
    dy_tokens = jax.random.normal(key_list[6], (ALL_TOKENS, MODEL_DIM), jnp.float32)
    return {
        "x_tokens": x_tokens.astype(jnp.bfloat16),
        "w_router": router_f.astype(jnp.bfloat16),
        "w_gate": w_gate.astype(jnp.bfloat16),
        "w_up": w_up.astype(jnp.bfloat16),
        "w_down": w_down.astype(jnp.bfloat16),
        "topk_idx": topk_idx,
        "dy_tokens": dy_tokens.astype(jnp.bfloat16),
    }


def reference(x_tokens, w_router, w_gate, w_up, w_down, topk_idx, dy_tokens):
    logits = jnp.dot(x_tokens, w_router, preferred_element_type=jnp.float32)
    router_prob = jax.nn.softmax(logits, axis=-1)
    counts = jax.ops.segment_sum(jnp.ones((ALL_TOKENS * TOP_K,), jnp.float32), topk_idx.reshape(-1), num_segments=NUM_EXPERTS)
    load_frac = counts / (ALL_TOKENS * TOP_K)
    mean_prob = jnp.mean(router_prob, axis=0)
    aux_loss = AUX_COEF * NUM_EXPERTS * jnp.sum(load_frac * mean_prob)
    aux_grad = AUX_COEF * NUM_EXPERTS * load_frac / ALL_TOKENS
    w_gate32 = w_gate.astype(jnp.float32)
    w_up32 = w_up.astype(jnp.float32)
    w_down32 = w_down.astype(jnp.float32)
    zero_row = jnp.zeros((1, MODEL_DIM), x_tokens.dtype)
    n_slots = NUM_EXPERTS * CAPACITY

    def device_step(carry_acc, dev_in):
        dwg_acc, dwu_acc, dwd_acc, dwr_acc = carry_acc
        x_dev, prob_dev, idx_dev, dy_dev = dev_in
        pick_prob = jnp.take_along_axis(prob_dev, idx_dev, axis=1)
        pick_sum = jnp.sum(pick_prob, axis=1, keepdims=True)
        gate_f32 = pick_prob / pick_sum
        gate_bf = gate_f32.astype(jnp.bfloat16)
        choice_mask = idx_dev[:, :, None] == jnp.arange(NUM_EXPERTS)[None, None, :]
        expert_hot = jnp.sum(choice_mask.astype(jnp.int32), axis=1)
        earlier = jnp.cumsum(expert_hot, axis=0) - expert_hot
        position = jnp.take_along_axis(earlier, idx_dev, axis=1)
        slot_ids = jnp.where(position < CAPACITY, idx_dev * CAPACITY + position, n_slots)
        flat_slots = slot_ids.reshape(-1)
        x_rep = jnp.broadcast_to(x_dev[:, None, :], (TOK_PER_DEV, TOP_K, MODEL_DIM)).reshape(TOK_PER_DEV * TOP_K, MODEL_DIM)
        buf_x = jnp.zeros((n_slots + 1, MODEL_DIM), x_dev.dtype).at[flat_slots].set(x_rep)[:n_slots]
        buf_x32 = buf_x.reshape(NUM_EXPERTS, CAPACITY, MODEL_DIM).astype(jnp.float32)
        gate_pre = jnp.einsum("ecd,edf->ecf", buf_x32, w_gate32)
        up_pre = jnp.einsum("ecd,edf->ecf", buf_x32, w_up32)
        act_gate = jax.nn.silu(gate_pre)
        hidden = (act_gate * up_pre).astype(jnp.bfloat16).astype(jnp.float32)
        out_slot = jnp.einsum("ecf,efd->ecd", hidden, w_down32).astype(jnp.bfloat16)
        out_tok = jnp.concatenate([out_slot.reshape(n_slots, MODEL_DIM), zero_row])[slot_ids]
        y_dev = jnp.sum(gate_bf.astype(jnp.float32)[:, :, None] * out_tok.astype(jnp.float32), axis=1).astype(jnp.bfloat16)
        do_tok = (gate_bf.astype(jnp.float32)[:, :, None] * dy_dev.astype(jnp.float32)[:, None, :]).astype(jnp.bfloat16)
        buf_do = jnp.zeros((n_slots + 1, MODEL_DIM), dy_dev.dtype).at[flat_slots].set(do_tok.reshape(TOK_PER_DEV * TOP_K, MODEL_DIM))[:n_slots]
        buf_do32 = buf_do.reshape(NUM_EXPERTS, CAPACITY, MODEL_DIM).astype(jnp.float32)
        dwd_new = dwd_acc + jnp.einsum("ecf,ecd->efd", hidden, buf_do32)
        d_hidden = jnp.einsum("ecd,efd->ecf", buf_do32, w_down32).astype(jnp.bfloat16).astype(jnp.float32)
        sigmoid_g = jax.nn.sigmoid(gate_pre)
        d_gate_pre = (d_hidden * up_pre * sigmoid_g * (1.0 + gate_pre * (1.0 - sigmoid_g))).astype(jnp.bfloat16).astype(jnp.float32)
        d_up_pre = (d_hidden * act_gate).astype(jnp.bfloat16).astype(jnp.float32)
        dwg_new = dwg_acc + jnp.einsum("ecd,ecf->edf", buf_x32, d_gate_pre)
        dwu_new = dwu_acc + jnp.einsum("ecd,ecf->edf", buf_x32, d_up_pre)
        dx_slot = (jnp.einsum("ecf,edf->ecd", d_gate_pre, w_gate32) + jnp.einsum("ecf,edf->ecd", d_up_pre, w_up32)).astype(jnp.bfloat16)
        dx_tok = jnp.concatenate([dx_slot.reshape(n_slots, MODEL_DIM), zero_row])[slot_ids]
        dx_expert = jnp.sum(dx_tok.astype(jnp.float32), axis=1)
        d_gate = jnp.sum(out_tok.astype(jnp.float32) * dy_dev.astype(jnp.float32)[:, None, :], axis=2)
        d_pick = (d_gate - jnp.sum(d_gate * gate_f32, axis=1, keepdims=True)) / pick_sum
        d_prob = jnp.sum(jnp.where(choice_mask, d_pick[:, :, None], 0.0), axis=1) + aux_grad
        d_logit = prob_dev * (d_prob - jnp.sum(prob_dev * d_prob, axis=1, keepdims=True))
        d_logit_bf = d_logit.astype(jnp.bfloat16)
        dwr_new = dwr_acc + jnp.dot(x_dev.T, d_logit_bf, preferred_element_type=jnp.float32)
        dx_dev = (dx_expert + jnp.dot(d_logit_bf, w_router.T, preferred_element_type=jnp.float32)).astype(jnp.bfloat16)
        return (dwg_new, dwu_new, dwd_new, dwr_new), (y_dev, dx_dev)

    init_acc = (
        jnp.zeros((NUM_EXPERTS, MODEL_DIM, FF_DIM), jnp.float32),
        jnp.zeros((NUM_EXPERTS, MODEL_DIM, FF_DIM), jnp.float32),
        jnp.zeros((NUM_EXPERTS, FF_DIM, MODEL_DIM), jnp.float32),
        jnp.zeros((MODEL_DIM, NUM_EXPERTS), jnp.float32),
    )
    dev_inputs = (
        x_tokens.reshape(NUM_DEVICES, TOK_PER_DEV, MODEL_DIM),
        router_prob.reshape(NUM_DEVICES, TOK_PER_DEV, NUM_EXPERTS),
        topk_idx.reshape(NUM_DEVICES, TOK_PER_DEV, TOP_K),
        dy_tokens.reshape(NUM_DEVICES, TOK_PER_DEV, MODEL_DIM),
    )
    final_acc, dev_outs = lax.scan(device_step, init_acc, dev_inputs)
    y_tokens = dev_outs[0].reshape(ALL_TOKENS, MODEL_DIM)
    dx_tokens = dev_outs[1].reshape(ALL_TOKENS, MODEL_DIM)
    return (y_tokens, aux_loss, dx_tokens, final_acc[3], final_acc[0], final_acc[1], final_acc[2])
```

```python
import functools

import jax
import jax.numpy as jnp
from jax import lax
from jax.experimental import pallas as pl
from jax.experimental.pallas import tpu as pltpu
from jax.sharding import PartitionSpec as P


AUX_COEF = 0.001
RING = (0, 1, 3, 2)
F32 = jnp.float32
BF16 = jnp.bfloat16


def device_perm(move):
    pairs = []
    for dev in range(32):
        z, y, x, core = move(dev // 8, (dev // 4) % 2, (dev // 2) % 2, dev % 2)
        pairs.append((dev, z * 8 + y * 4 + x * 2 + core))
    return pairs


RING_NEXT = {RING[i]: RING[(i + 1) % 4] for i in range(4)}
PERM_Z = device_perm(lambda z, y, x, c: (RING_NEXT[z], y, x, c))
PERM_X = device_perm(lambda z, y, x, c: (z, y, 1 - x, c))
PERM_Y = device_perm(lambda z, y, x, c: (z, 1 - y, x, c))
PERM_D = device_perm(lambda z, y, x, c: (z, 1 - y, 1 - x, c))
PERM_C = device_perm(lambda z, y, x, c: (z, y, x, 1 - c))


def send(value, perm):
    return lax.ppermute(value, "ep", perm)


def dot_nt(lhs, rhs):
    return lax.dot_general(lhs, rhs, (((1,), (1,)), ((), ())), preferred_element_type=F32)


def dot_tn(lhs, rhs):
    return lax.dot_general(lhs, rhs, (((0,), (0,)), ((), ())), preferred_element_type=F32)


def dot_nn(lhs, rhs):
    return jnp.dot(lhs, rhs, preferred_element_type=F32)


def params(limit_mib=60, **kwargs):
    return pltpu.CompilerParams(vmem_limit_bytes=limit_mib * 1024 * 1024, **kwargs)


def chosen_mask(idx_ref, n_exp, tok_count):
    expert_iota = lax.broadcasted_iota(jnp.int32, (n_exp, tok_count), 0)
    hot = jnp.zeros((n_exp, tok_count), F32)
    for k in range(idx_ref.shape[0]):
        hot = hot + jnp.where(expert_iota == idx_ref[k:k + 1, :], 1.0, 0.0)
    return hot


def route_kernel(capacity, x_ref, wr_ref, idx_ref, prob_ref, meta_ref, stat_ref):
    n_exp, tok_count = prob_ref.shape
    logits = lax.dot_general(wr_ref[...], x_ref[...], (((0,), (1,)), ((), ())), preferred_element_type=F32)
    expo = jnp.exp(logits - jnp.max(logits, axis=0, keepdims=True))
    prob = expo / jnp.sum(expo, axis=0, keepdims=True)
    prob_ref[...] = prob
    hot = chosen_mask(idx_ref, n_exp, tok_count)
    pick = hot * prob
    gate = pick / jnp.sum(pick, axis=0, keepdims=True)
    hot_bf = hot.astype(BF16)
    row = lax.broadcasted_iota(jnp.int32, (tok_count, 256), 0)
    lane = lax.broadcasted_iota(jnp.int32, (tok_count, 256), 1)
    for block in range(tok_count // 256):
        span = slice(block * 256, (block + 1) * 256)
        before = jnp.where(row < lane + block * 256, 1.0, 0.0).astype(BF16)
        earlier = dot_nn(hot_bf, before)
        keep = (hot[:, span] > 0.5) & (earlier < capacity)
        meta_ref[0:n_exp, span] = jnp.where(keep, earlier, -1.0)
    meta_ref[n_exp:2 * n_exp, :] = gate.astype(BF16).astype(F32)
    count = jnp.sum(hot, axis=1, keepdims=True)
    total = jnp.sum(prob, axis=1, keepdims=True)
    lanes = lax.broadcasted_iota(jnp.int32, (n_exp, tok_count), 1)
    stat_ref[...] = jnp.where(lanes < tok_count // 2, count, total)


def gather_kernel(capacity, eid_ref, x_ref, dy_ref, meta_ref, xs_ref, dr_ref, ws_ref, pos_ref, gate_ref):
    step = pl.program_id(0)
    n_exp = meta_ref.shape[0] // 2
    tok_count = x_ref.shape[0]
    slot = lax.broadcasted_iota(jnp.int32, (capacity, tok_count), 0).astype(F32)
    picks = []
    for b in range(2):
        j = step * 2 + b
        expert = eid_ref[j]
        pos = meta_ref[pl.ds(expert, 1), :]
        gate = meta_ref[pl.ds(expert + n_exp, 1), :]
        pos_ref[pl.ds(j, 1), :] = pos
        gate_ref[pl.ds(j, 1), :] = gate
        match = slot == pos
        weight = jnp.sum(jnp.where(match, gate, 0.0), axis=1, keepdims=True)
        ws_ref[b * capacity:(b + 1) * capacity, :] = jnp.broadcast_to(weight, (capacity, 128))
        picks.append(jnp.where(match, 1.0, 0.0).astype(BF16))
    pick = jnp.concatenate(picks, axis=0)
    xs_ref[...] = dot_nn(pick, x_ref[...]).astype(BF16)
    dr_ref[...] = dot_nn(pick, dy_ref[...]).astype(BF16)


def expert_kernel(slot_j, capacity, *refs):
    n_blk = 4
    xs, dr, ws, pos = refs[0:4], refs[4:8], refs[8:12], refs[12:16]
    wg, wu, wd = refs[16:19]
    o_out, dx_out, a_out, dwg_out, dwu_out, dwd_out = refs[19:25]
    (xs_v, dr_v, ws_v, pos_v, wg_v, wu_v, wd_v, o_v, dx_v, d_v, h_v, dg_v, du_v,
     dwg_v, dwu_v, dwd_v, in_sem, w_sem, out_sem, dw_sem) = refs[25:]
    tok_count = pos_v.shape[1]

    def weight_copies():
        pairs = ((wg, wg_v), (wu, wu_v), (wd, wd_v))
        return [pltpu.make_async_copy(src, dst, w_sem.at[i]) for i, (src, dst) in enumerate(pairs)]

    def row_copies(t, src_t):
        src = pl.ds(slot_j * capacity, capacity)
        dst = pl.ds(t * capacity, capacity)
        return [
            pltpu.make_async_copy(xs[src_t].at[src], xs_v.at[dst], in_sem.at[t, 0]),
            pltpu.make_async_copy(dr[src_t].at[src], dr_v.at[dst], in_sem.at[t, 1]),
            pltpu.make_async_copy(ws[src_t].at[src], ws_v.at[dst], in_sem.at[t, 2]),
        ]

    def out_copies(t):
        src = pl.ds(t * capacity, capacity)
        return [
            pltpu.make_async_copy(o_v.at[src], o_out.at[t], out_sem.at[t, 0]),
            pltpu.make_async_copy(dx_v.at[src], dx_out.at[t], out_sem.at[t, 1]),
        ]

    def dw_copies():
        pairs = ((dwg_v, dwg_out), (dwu_v, dwu_out), (dwd_v, dwd_out))
        return [pltpu.make_async_copy(src, dst, dw_sem.at[i]) for i, (src, dst) in enumerate(pairs)]

    for copy in weight_copies()[:2]:
        copy.start()
    for t in range(n_blk):
        for copy in row_copies(t, t):
            copy.start()
        if t == 0:
            weight_copies()[2].start()
    for t in range(n_blk):
        pos_v[t:t + 1, :] = pos[t][slot_j:slot_j + 1, :]
    slot = lax.broadcasted_iota(jnp.int32, (capacity, tok_count), 0).astype(F32)
    for copy in weight_copies():
        copy.wait()

    def block_body(t, carry):
        for copy in row_copies(t, 0):
            copy.wait()
        rows = pl.ds(pl.multiple_of(t * capacity, 64), capacity)
        x = xs_v[rows, :]
        g = dot_nn(x, wg_v[...])
        u = dot_nn(x, wu_v[...])
        sig = jax.nn.sigmoid(g)
        act = g * sig
        h = (act * u).astype(BF16)
        h_v[rows, :] = h
        o = dot_nn(h, wd_v[...]).astype(BF16)
        o_v[rows, :] = o
        d_raw = dr_v[rows, :].astype(F32)
        a = jnp.sum(o.astype(F32) * d_raw, axis=1, keepdims=True)
        a_out[pl.ds(t, 1), :] = jnp.sum(jnp.where(slot == pos_v[pl.ds(t, 1), :], a, 0.0), axis=0, keepdims=True)
        d = (ws_v[rows, 0:1] * d_raw).astype(BF16)
        d_v[rows, :] = d
        dh = dot_nt(d, wd_v[...]).astype(BF16).astype(F32)
        dg = (dh * u * sig * (1.0 + g * (1.0 - sig))).astype(BF16)
        du = (dh * act).astype(BF16)
        dg_v[rows, :] = dg
        du_v[rows, :] = du
        dx_v[rows, :] = (dot_nt(dg, wg_v[...]) + dot_nt(du, wu_v[...])).astype(BF16)
        for copy in out_copies(t):
            copy.start()
        return carry

    lax.fori_loop(0, n_blk, block_body, 0)

    def gate_body(m, carry):
        cols = pl.ds(pl.multiple_of(m * 256, 256), 256)
        x = xs_v[:, cols]
        dwg_v[cols, :] = dot_tn(x, dg_v[...])
        dwu_v[cols, :] = dot_tn(x, du_v[...])
        return carry

    lax.fori_loop(0, xs_v.shape[1] // 256, gate_body, 0)
    for copy in dw_copies()[:2]:
        copy.start()

    def down_body(m, carry):
        cols = pl.ds(pl.multiple_of(m * 256, 256), 256)
        dwd_v[cols, :] = dot_tn(h_v[:, cols], d_v[...])
        return carry

    lax.fori_loop(0, h_v.shape[1] // 256, down_body, 0)
    dw_copies()[2].start()
    for t in range(n_blk):
        for copy in out_copies(t):
            copy.wait()
    for copy in dw_copies():
        copy.wait()


def combine_kernel(capacity, *refs):
    o_refs, dx_refs = refs[0:8], refs[8:16]
    pos_ref, gate_ref, y_ref, dxo_ref = refs[16:]
    rows = y_ref.shape[0]
    start = pl.multiple_of(pl.program_id(0) * rows, rows)
    pos = pos_ref[:, pl.ds(start, rows)].T
    gate = gate_ref[:, pl.ds(start, rows)].T
    lane = lax.broadcasted_iota(jnp.int32, (rows, 2 * capacity), 1).astype(F32)
    first = lane < capacity
    y_acc = jnp.zeros(y_ref.shape, F32)
    dx_acc = jnp.zeros(y_ref.shape, F32)
    for k in range(4):
        pos_a, pos_b = pos[:, 2 * k:2 * k + 1], pos[:, 2 * k + 1:2 * k + 2]
        pos_b = jnp.where(pos_b < 0.0, -1.0, pos_b + capacity)
        match = lane == jnp.where(first, pos_a, pos_b)
        weight = jnp.where(first, gate[:, 2 * k:2 * k + 1], gate[:, 2 * k + 1:2 * k + 2])
        pick_w = jnp.where(match, weight, 0.0).astype(BF16)
        pick_1 = jnp.where(match, 1.0, 0.0).astype(BF16)
        o_pair = jnp.concatenate([o_refs[2 * k][0], o_refs[2 * k + 1][0]], axis=0)
        dx_pair = jnp.concatenate([dx_refs[2 * k][0], dx_refs[2 * k + 1][0]], axis=0)
        y_acc = y_acc + dot_nn(pick_w, o_pair)
        dx_acc = dx_acc + dot_nn(pick_1, dx_pair)
    y_ref[...] = y_acc
    dxo_ref[...] = dx_acc


def router_kernel(aux_scale, eid_ref, a0, a1, a2, a3, prob_ref, idx_ref, frac_ref, wr_ref, x_ref, dwr_ref, dxr_ref, a_v):
    n_exp, tok_count = prob_ref.shape
    for q, a_ref in enumerate((a0, a1, a2, a3)):
        for j in range(8):
            a_v[pl.ds(eid_ref[q * 8 + j], 1), :] = a_ref[j:j + 1, :]
    prob = prob_ref[...]
    a = a_v[...]
    hot = chosen_mask(idx_ref, n_exp, tok_count)
    pick = hot * prob
    pick_sum = jnp.sum(pick, axis=0, keepdims=True)
    gate = pick / pick_sum
    d_pick = (a - jnp.sum(a * gate, axis=0, keepdims=True)) / pick_sum
    d_prob = jnp.where(hot > 0.5, d_pick, 0.0) + aux_scale * frac_ref[...]
    dz = (prob * (d_prob - jnp.sum(prob * d_prob, axis=0, keepdims=True))).astype(BF16)
    dwr_ref[...] = dot_nn(dz, x_ref[...])
    dxr_ref[...] = lax.dot_general(dz, wr_ref[...], (((0,), (1,)), ((), ())), preferred_element_type=F32)


def cost(flops, nbytes):
    return pl.CostEstimate(flops=int(flops), bytes_accessed=int(nbytes), transcendentals=0)


def make_calls(capacity, tok_count, model_dim, ff_dim, n_exp):
    vmem = pl.BlockSpec(memory_space=pltpu.VMEM)
    smem = pl.BlockSpec(memory_space=pltpu.SMEM)
    hbm = pl.BlockSpec(memory_space=pl.ANY)
    shape = jax.ShapeDtypeStruct
    n_rows = 4 * capacity
    small = pl.BlockSpec((8, tok_count), lambda i: (0, 0))

    def gather(eid, x, dy, meta):
        rows = 2 * capacity
        full = pl.BlockSpec((tok_count, model_dim), lambda i: (0, 0))
        out = pl.BlockSpec((rows, model_dim), lambda i: (i, 0))
        slots = shape((8 * capacity, model_dim), BF16)
        vec = shape((8, tok_count), F32)
        return pl.pallas_call(
            functools.partial(gather_kernel, capacity), grid=(4,),
            out_shape=(slots, slots, shape((8 * capacity, 128), F32), vec, vec),
            in_specs=[smem, full, full, pl.BlockSpec((2 * n_exp, tok_count), lambda i: (0, 0))],
            out_specs=(out, out, pl.BlockSpec((rows, 128), lambda i: (i, 0)), small, small),
            compiler_params=params(dimension_semantics=("arbitrary",)),
            cost_estimate=cost(32 * capacity * tok_count * model_dim, 16e6), name="gather",
        )(eid, x, dy, meta)

    def experts(j, *args):
        slots = shape((4, capacity, model_dim), BF16)
        dw_in, dw_out = shape((model_dim, ff_dim), F32), shape((ff_dim, model_dim), F32)
        wide, narrow = pltpu.VMEM((n_rows, model_dim), BF16), pltpu.VMEM((n_rows, ff_dim), BF16)
        return pl.pallas_call(
            functools.partial(expert_kernel, j, capacity),
            out_shape=(slots, slots, shape((4, tok_count), F32), dw_in, dw_in, dw_out),
            in_specs=[hbm] * 12 + [vmem] * 4 + [hbm] * 3,
            out_specs=(hbm, hbm, vmem, hbm, hbm, hbm),
            scratch_shapes=[
                wide, wide, pltpu.VMEM((n_rows, 128), F32), pltpu.VMEM((4, tok_count), F32),
                pltpu.VMEM((model_dim, ff_dim), BF16), pltpu.VMEM((model_dim, ff_dim), BF16),
                pltpu.VMEM((ff_dim, model_dim), BF16), wide, wide, wide, narrow, narrow, narrow,
                pltpu.VMEM((model_dim, ff_dim), F32), pltpu.VMEM((model_dim, ff_dim), F32),
                pltpu.VMEM((ff_dim, model_dim), F32),
                pltpu.SemaphoreType.DMA((4, 3)), pltpu.SemaphoreType.DMA((3,)),
                pltpu.SemaphoreType.DMA((4, 2)), pltpu.SemaphoreType.DMA((3,)),
            ],
            compiler_params=params(56), cost_estimate=cost(18 * n_rows * model_dim * ff_dim, 20e6), name="experts",
        )(*args)

    def combine(t, *args):
        tile = 256
        pick = pl.BlockSpec((1, capacity, model_dim), lambda i: (t, 0, 0))
        out = pl.BlockSpec((tile, model_dim), lambda i: (i, 0))
        return pl.pallas_call(
            functools.partial(combine_kernel, capacity), grid=(tok_count // tile,),
            out_shape=(shape((tok_count, model_dim), F32),) * 2,
            in_specs=[pick] * 16 + [small] * 2, out_specs=(out, out),
            compiler_params=params(dimension_semantics=("arbitrary",)),
            cost_estimate=cost(32 * capacity * tok_count * model_dim, 20e6), name="combine",
        )(*args)

    return gather, experts, combine


def solution(mesh):
    n_dev = mesh.shape["ep"]

    def block_body(x_loc, w_router, wg_loc, wu_loc, wd_loc, idx_loc, dy_loc):
        tok_count, model_dim = x_loc.shape
        top_k = idx_loc.shape[1]
        n_exp = w_router.shape[1]
        ff_dim = wg_loc.shape[2]
        capacity = (5 * tok_count * top_k + 4 * n_exp - 1) // (4 * n_exp)
        n_total = tok_count * n_dev
        vmem = pl.BlockSpec(memory_space=pltpu.VMEM)
        smem = pl.BlockSpec(memory_space=pltpu.SMEM)
        shape = jax.ShapeDtypeStruct
        me = lax.axis_index("ep")
        core = me % 2
        column = (me // 2) % 4
        ring_pos = jnp.array([0, 1, 3, 2], jnp.int32)[me // 8]
        ring_arr = jnp.array(RING, jnp.int32)

        def expert_ids(col):
            dist = jnp.arange(4, dtype=jnp.int32)
            z_of = ring_arr[(ring_pos - dist + 4) % 4]
            base = z_of * 8 + col * 2
            return jnp.stack([base + core, base + 1 - core], axis=1).reshape(8)

        eid = expert_ids(column)
        eid_all = jnp.concatenate([eid, expert_ids(column ^ 1), expert_ids(column ^ 2), expert_ids(column ^ 3)])
        idx_t = idx_loc.T

        x_x, dy_x = send(x_loc, PERM_X), send(dy_loc, PERM_X)
        x_y, dy_y = send(x_loc, PERM_Y), send(dy_loc, PERM_Y)
        x_d, dy_d = send(x_x, PERM_Y), send(dy_y, PERM_X)
        xs_all = (x_loc, x_x, x_y, x_d)
        dys_all = (dy_loc, dy_x, dy_y, dy_d)

        mine = [(wg_loc[0], wu_loc[0], wd_loc[0])]
        for _ in range(3):
            mine.append(tuple(send(w, PERM_Z) for w in mine[-1]))
        other = [tuple(send(w, PERM_C) for w in ws) for ws in mine]

        prob, meta, stat = pl.pallas_call(
            functools.partial(route_kernel, capacity),
            out_shape=(shape((n_exp, tok_count), F32), shape((2 * n_exp, tok_count), F32), shape((n_exp, tok_count), F32)),
            in_specs=[vmem] * 3, out_specs=(vmem,) * 3, compiler_params=params(),
            cost_estimate=cost(4e9, 4e6), name="route",
        )(x_loc, w_router, idx_t)
        stat = lax.psum(stat, "ep")
        meta_x, meta_y = send(meta, PERM_X), send(meta, PERM_Y)
        meta_d = send(meta, PERM_D)
        load_frac = stat[:, 0:1] / (n_total * top_k)
        mean_prob = stat[:, tok_count - 1:] / n_total
        aux_loss = AUX_COEF * n_exp * jnp.sum(load_frac * mean_prob)

        gather, expert_call, combine_call = make_calls(capacity, tok_count, model_dim, ff_dim, n_exp)
        metas = (meta, meta_x, meta_y, meta_d)
        gathered = [gather(eid, x, dy, m) for x, dy, m in zip(xs_all, dys_all, metas)]
        xs, dr, ws, pos, gate = zip(*gathered)

        o_j, dx_j, a_j = [None] * 8, [None] * 8, [None] * 8
        travel = None
        for k in (1, 2, 3, 0):
            j = 2 * k + 1
            o_j[j], dx_j[j], a_j[j], *dw_other = expert_call(j, *xs, *dr, *ws, *pos, *other[k])
            dw_sib = [send(part, PERM_C) for part in dw_other]
            j = 2 * k
            o_j[j], dx_j[j], a_j[j], *dw_mine = expert_call(j, *xs, *dr, *ws, *pos, *mine[k])
            total = [own + sib for own, sib in zip(dw_mine, dw_sib)]
            if travel is not None:
                total = [part + came for part, came in zip(total, travel)]
            travel = [send(part, PERM_Z) for part in total] if k else total
        dw_gate, dw_up, dw_down = (part[None] for part in travel)

        def combine(t):
            return combine_call(t, *o_j, *dx_j, pos[t], gate[t])

        y_d, dx_d = combine(3)
        y_d_in, dx_d_in = send(y_d, PERM_X), send(dx_d, PERM_Y)
        y_x, dx_x = combine(1)
        y_x_in = send(y_x, PERM_X)
        y_y, dx_y = combine(2)
        dx_y_in = send(dx_y, PERM_Y)
        y_y_in = send(y_y + y_d_in, PERM_Y)
        dx_x_in = send(dx_x + dx_d_in, PERM_X)
        y_0, dx_0 = combine(0)

        def a_rows(t):
            return jnp.concatenate([a_j[j][t:t + 1] for j in range(8)], axis=0)

        a_in = [a_rows(0), send(a_rows(1), PERM_X), send(a_rows(2), PERM_Y), send(a_rows(3), PERM_D)]
        dwr_t, dx_r = pl.pallas_call(
            functools.partial(router_kernel, AUX_COEF * n_exp / n_total),
            out_shape=(shape((n_exp, model_dim), F32), shape((tok_count, model_dim), F32)),
            in_specs=[smem] + [vmem] * 9, out_specs=(vmem,) * 2,
            scratch_shapes=[pltpu.VMEM((n_exp, tok_count), F32)],
            compiler_params=params(), cost_estimate=cost(1e9, 8e6), name="router",
        )(eid_all, *a_in, prob, idx_t, load_frac, w_router, x_loc)
        dw_router = lax.psum(dwr_t, "ep").T
        y_loc = (y_0 + y_x_in + y_y_in).astype(BF16)
        dx_loc = (dx_0 + dx_y_in + dx_x_in + dx_r).astype(BF16)
        return y_loc, aux_loss, dx_loc, dw_router, dw_gate, dw_up, dw_down

    tok_spec = P("ep")
    return jax.shard_map(
        block_body,
        mesh=mesh,
        in_specs=(tok_spec, P(), tok_spec, tok_spec, tok_spec, tok_spec, tok_spec),
        out_specs=(tok_spec, P(), tok_spec, P(), tok_spec, tok_spec, tok_spec),
        check_vma=False,
    )
```

```python
import functools

import jax
import jax.numpy as jnp
from jax import lax
from jax.experimental import pallas as pl
from jax.experimental.pallas import tpu as pltpu
from jax.sharding import PartitionSpec as P


AUX_COEF = 0.001
RING = (0, 1, 3, 2)
F32 = jnp.float32
BF16 = jnp.bfloat16


def device_perm(move):
    pairs = []
    for dev in range(32):
        z, y, x, core = move(dev // 8, (dev // 4) % 2, (dev // 2) % 2, dev % 2)
        pairs.append((dev, z * 8 + y * 4 + x * 2 + core))
    return pairs


RING_NEXT = {RING[i]: RING[(i + 1) % 4] for i in range(4)}
PERM_Z = device_perm(lambda z, y, x, c: (RING_NEXT[z], y, x, c))
PERM_X = device_perm(lambda z, y, x, c: (z, y, 1 - x, c))
PERM_Y = device_perm(lambda z, y, x, c: (z, 1 - y, x, c))
PERM_D = device_perm(lambda z, y, x, c: (z, 1 - y, 1 - x, c))
PERM_C = device_perm(lambda z, y, x, c: (z, y, x, 1 - c))


def send(value, perm):
    return lax.ppermute(value, "ep", perm)


def dot_nt(lhs, rhs):
    return lax.dot_general(lhs, rhs, (((1,), (1,)), ((), ())), preferred_element_type=F32)


def dot_tn(lhs, rhs):
    return lax.dot_general(lhs, rhs, (((0,), (0,)), ((), ())), preferred_element_type=F32)


def dot_nn(lhs, rhs):
    return jnp.dot(lhs, rhs, preferred_element_type=F32)


def params(limit_mib=60, **kwargs):
    return pltpu.CompilerParams(vmem_limit_bytes=limit_mib * 1024 * 1024, **kwargs)


def chosen_mask(idx_ref, n_exp, tok_count):
    expert_iota = lax.broadcasted_iota(jnp.int32, (n_exp, tok_count), 0)
    hot = jnp.zeros((n_exp, tok_count), F32)
    for k in range(idx_ref.shape[0]):
        hot = hot + jnp.where(expert_iota == idx_ref[k:k + 1, :], 1.0, 0.0)
    return hot


def route_kernel(capacity, x_ref, wr_ref, idx_ref, prob_ref, meta_ref, stat_ref):
    n_exp, tok_count = prob_ref.shape
    logits = lax.dot_general(wr_ref[...], x_ref[...], (((0,), (1,)), ((), ())), preferred_element_type=F32)
    expo = jnp.exp(logits - jnp.max(logits, axis=0, keepdims=True))
    prob = expo / jnp.sum(expo, axis=0, keepdims=True)
    prob_ref[...] = prob
    hot = chosen_mask(idx_ref, n_exp, tok_count)
    pick = hot * prob
    gate = pick / jnp.sum(pick, axis=0, keepdims=True)
    hot_bf = hot.astype(BF16)
    row = lax.broadcasted_iota(jnp.int32, (tok_count, 256), 0)
    lane = lax.broadcasted_iota(jnp.int32, (tok_count, 256), 1)
    for block in range(tok_count // 256):
        span = slice(block * 256, (block + 1) * 256)
        before = jnp.where(row < lane + block * 256, 1.0, 0.0).astype(BF16)
        earlier = dot_nn(hot_bf, before)
        keep = (hot[:, span] > 0.5) & (earlier < capacity)
        meta_ref[0:n_exp, span] = jnp.where(keep, earlier, -1.0)
    meta_ref[n_exp:2 * n_exp, :] = gate.astype(BF16).astype(F32)
    count = jnp.sum(hot, axis=1, keepdims=True)
    total = jnp.sum(prob, axis=1, keepdims=True)
    lanes = lax.broadcasted_iota(jnp.int32, (n_exp, tok_count), 1)
    stat_ref[...] = jnp.where(lanes < tok_count // 2, count, total)


def gather_kernel(capacity, eid_ref, x_ref, dy_ref, meta_ref, xs_ref, dr_ref, ws_ref, pos_ref, gate_ref):
    step = pl.program_id(0)
    n_exp = meta_ref.shape[0] // 2
    tok_count = x_ref.shape[0]
    slot = lax.broadcasted_iota(jnp.int32, (capacity, tok_count), 0).astype(F32)
    picks = []
    for b in range(2):
        j = step * 2 + b
        expert = eid_ref[j]
        pos = meta_ref[pl.ds(expert, 1), :]
        gate = meta_ref[pl.ds(expert + n_exp, 1), :]
        pos_ref[pl.ds(j, 1), :] = pos
        gate_ref[pl.ds(j, 1), :] = gate
        match = slot == pos
        weight = jnp.sum(jnp.where(match, gate, 0.0), axis=1, keepdims=True)
        ws_ref[b * capacity:(b + 1) * capacity, :] = jnp.broadcast_to(weight, (capacity, 128))
        picks.append(jnp.where(match, 1.0, 0.0).astype(BF16))
    pick = jnp.concatenate(picks, axis=0)
    xs_ref[...] = dot_nn(pick, x_ref[...]).astype(BF16)
    dr_ref[...] = dot_nn(pick, dy_ref[...]).astype(BF16)


def expert_kernel(slot_j, capacity, *refs):
    n_blk = 4
    xs, dr, ws, pos = refs[0:4], refs[4:8], refs[8:12], refs[12:16]
    wg, wu, wd = refs[16:19]
    o_out, dx_out, a_out, dwg_out, dwu_out, dwd_out = refs[19:25]
    (xs_v, dr_v, ws_v, pos_v, wg_v, wu_v, wd_v, o_v, dx_v, d_v, h_v, dg_v, du_v,
     dwg_v, dwu_v, dwd_v, in_sem, w_sem, out_sem, dw_sem) = refs[25:]
    tok_count = pos_v.shape[1]

    def weight_copies():
        pairs = ((wg, wg_v), (wu, wu_v), (wd, wd_v))
        return [pltpu.make_async_copy(src, dst, w_sem.at[i]) for i, (src, dst) in enumerate(pairs)]

    def row_copies(t, src_t):
        src = pl.ds(slot_j * capacity, capacity)
        dst = pl.ds(t * capacity, capacity)
        return [
            pltpu.make_async_copy(xs[src_t].at[src], xs_v.at[dst], in_sem.at[t, 0]),
            pltpu.make_async_copy(dr[src_t].at[src], dr_v.at[dst], in_sem.at[t, 1]),
            pltpu.make_async_copy(ws[src_t].at[src], ws_v.at[dst], in_sem.at[t, 2]),
        ]

    def out_copies(t):
        src = pl.ds(t * capacity, capacity)
        return [
            pltpu.make_async_copy(o_v.at[src], o_out.at[t], out_sem.at[t, 0]),
            pltpu.make_async_copy(dx_v.at[src], dx_out.at[t], out_sem.at[t, 1]),
        ]

    def dw_copies():
        pairs = ((dwg_v, dwg_out), (dwu_v, dwu_out), (dwd_v, dwd_out))
        return [pltpu.make_async_copy(src, dst, dw_sem.at[i]) for i, (src, dst) in enumerate(pairs)]

    first = row_copies(0, 0)
    loads = weight_copies()
    for copy in (first[0], loads[0], loads[1], first[1], first[2], loads[2], *row_copies(1, 1)):
        copy.start()
    for t in range(n_blk):
        pos_v[t:t + 1, :] = pos[t][slot_j:slot_j + 1, :]
    slot = lax.broadcasted_iota(jnp.int32, (capacity, tok_count), 0).astype(F32)
    for copy in loads[:2]:
        copy.wait()

    def block_body(t, carry):
        for later in range(2, n_blk):
            @pl.when(t == later - 2)
            def _():
                for copy in row_copies(later, later):
                    copy.start()

        copy_x, copy_dy, copy_w = row_copies(t, 0)
        copy_x.wait()
        rows = pl.ds(pl.multiple_of(t * capacity, 64), capacity)
        x = xs_v[rows, :]
        g = dot_nn(x, wg_v[...])
        u = dot_nn(x, wu_v[...])
        sig = jax.nn.sigmoid(g)
        act = g * sig
        h = (act * u).astype(BF16)
        h_v[rows, :] = h

        @pl.when(t == 0)
        def _():
            loads[2].wait()

        copy_dy.wait()
        copy_w.wait()
        o = dot_nn(h, wd_v[...]).astype(BF16)
        o_v[rows, :] = o
        d_raw = dr_v[rows, :].astype(F32)
        a = jnp.sum(o.astype(F32) * d_raw, axis=1, keepdims=True)
        a_out[pl.ds(t, 1), :] = jnp.sum(jnp.where(slot == pos_v[pl.ds(t, 1), :], a, 0.0), axis=0, keepdims=True)
        d = (ws_v[rows, 0:1] * d_raw).astype(BF16)
        d_v[rows, :] = d
        dh = dot_nt(d, wd_v[...]).astype(BF16).astype(F32)
        dg = (dh * u * sig * (1.0 + g * (1.0 - sig))).astype(BF16)
        du = (dh * act).astype(BF16)
        dg_v[rows, :] = dg
        du_v[rows, :] = du
        dx_v[rows, :] = (dot_nt(dg, wg_v[...]) + dot_nt(du, wu_v[...])).astype(BF16)
        for copy in out_copies(t):
            copy.start()
        return carry

    lax.fori_loop(0, n_blk, block_body, 0)

    def gate_body(m, carry):
        cols = pl.ds(pl.multiple_of(m * 256, 256), 256)
        x = xs_v[:, cols]
        dwg_v[cols, :] = dot_tn(x, dg_v[...])
        dwu_v[cols, :] = dot_tn(x, du_v[...])
        return carry

    lax.fori_loop(0, xs_v.shape[1] // 256, gate_body, 0)
    stores = dw_copies()
    for copy in stores[:2]:
        copy.start()

    def down_body(m, carry):
        cols = pl.ds(pl.multiple_of(m * 256, 256), 256)
        dwd_v[cols, :] = dot_tn(h_v[:, cols], d_v[...])
        return carry

    lax.fori_loop(0, h_v.shape[1] // 256, down_body, 0)
    stores[2].start()
    for t in range(n_blk):
        for copy in out_copies(t):
            copy.wait()
    for copy in stores:
        copy.wait()


def combine_kernel(capacity, *refs):
    o_refs, dx_refs = refs[0:8], refs[8:16]
    pos_ref, gate_ref, y_ref, dxo_ref = refs[16:]
    rows = y_ref.shape[0]
    start = pl.multiple_of(pl.program_id(0) * rows, rows)
    pos = pos_ref[:, pl.ds(start, rows)].T
    gate = gate_ref[:, pl.ds(start, rows)].T
    lane = lax.broadcasted_iota(jnp.int32, (rows, 2 * capacity), 1).astype(F32)
    first = lane < capacity
    y_acc = jnp.zeros(y_ref.shape, F32)
    dx_acc = jnp.zeros(y_ref.shape, F32)
    for k in range(4):
        pos_a, pos_b = pos[:, 2 * k:2 * k + 1], pos[:, 2 * k + 1:2 * k + 2]
        pos_b = jnp.where(pos_b < 0.0, -1.0, pos_b + capacity)
        match = lane == jnp.where(first, pos_a, pos_b)
        weight = jnp.where(first, gate[:, 2 * k:2 * k + 1], gate[:, 2 * k + 1:2 * k + 2])
        pick_w = jnp.where(match, weight, 0.0).astype(BF16)
        pick_1 = jnp.where(match, 1.0, 0.0).astype(BF16)
        o_pair = jnp.concatenate([o_refs[2 * k][0], o_refs[2 * k + 1][0]], axis=0)
        dx_pair = jnp.concatenate([dx_refs[2 * k][0], dx_refs[2 * k + 1][0]], axis=0)
        y_acc = y_acc + dot_nn(pick_w, o_pair)
        dx_acc = dx_acc + dot_nn(pick_1, dx_pair)
    y_ref[...] = y_acc
    dxo_ref[...] = dx_acc


def router_kernel(aux_scale, eid_ref, a0, a1, a2, a3, prob_ref, idx_ref, frac_ref, wr_ref, x_ref, dwr_ref, dxr_ref, a_v):
    n_exp, tok_count = prob_ref.shape
    for q, a_ref in enumerate((a0, a1, a2, a3)):
        for j in range(8):
            a_v[pl.ds(eid_ref[q * 8 + j], 1), :] = a_ref[j:j + 1, :]
    prob = prob_ref[...]
    a = a_v[...]
    hot = chosen_mask(idx_ref, n_exp, tok_count)
    pick = hot * prob
    pick_sum = jnp.sum(pick, axis=0, keepdims=True)
    gate = pick / pick_sum
    d_pick = (a - jnp.sum(a * gate, axis=0, keepdims=True)) / pick_sum
    d_prob = jnp.where(hot > 0.5, d_pick, 0.0) + aux_scale * frac_ref[...]
    dz = (prob * (d_prob - jnp.sum(prob * d_prob, axis=0, keepdims=True))).astype(BF16)
    dwr_ref[...] = dot_nn(dz, x_ref[...])
    dxr_ref[...] = lax.dot_general(dz, wr_ref[...], (((0,), (1,)), ((), ())), preferred_element_type=F32)


def cost(flops, nbytes):
    return pl.CostEstimate(flops=int(flops), bytes_accessed=int(nbytes), transcendentals=0)


def make_calls(capacity, tok_count, model_dim, ff_dim, n_exp):
    vmem = pl.BlockSpec(memory_space=pltpu.VMEM)
    smem = pl.BlockSpec(memory_space=pltpu.SMEM)
    hbm = pl.BlockSpec(memory_space=pl.ANY)
    shape = jax.ShapeDtypeStruct
    n_rows = 4 * capacity
    small = pl.BlockSpec((8, tok_count), lambda i: (0, 0))

    def gather(eid, x, dy, meta):
        rows = 2 * capacity
        full = pl.BlockSpec((tok_count, model_dim), lambda i: (0, 0))
        out = pl.BlockSpec((rows, model_dim), lambda i: (i, 0))
        slots = shape((8 * capacity, model_dim), BF16)
        vec = shape((8, tok_count), F32)
        return pl.pallas_call(
            functools.partial(gather_kernel, capacity), grid=(4,),
            out_shape=(slots, slots, shape((8 * capacity, 128), F32), vec, vec),
            in_specs=[smem, full, full, pl.BlockSpec((2 * n_exp, tok_count), lambda i: (0, 0))],
            out_specs=(out, out, pl.BlockSpec((rows, 128), lambda i: (i, 0)), small, small),
            compiler_params=params(dimension_semantics=("arbitrary",)),
            cost_estimate=cost(32 * capacity * tok_count * model_dim, 16e6), name="gather",
        )(eid, x, dy, meta)

    def experts(j, *args):
        slots = shape((4, capacity, model_dim), BF16)
        dw_in, dw_out = shape((model_dim, ff_dim), F32), shape((ff_dim, model_dim), F32)
        wide, narrow = pltpu.VMEM((n_rows, model_dim), BF16), pltpu.VMEM((n_rows, ff_dim), BF16)
        return pl.pallas_call(
            functools.partial(expert_kernel, j, capacity),
            out_shape=(slots, slots, shape((4, tok_count), F32), dw_in, dw_in, dw_out),
            in_specs=[hbm] * 12 + [vmem] * 4 + [hbm] * 3,
            out_specs=(hbm, hbm, vmem, hbm, hbm, hbm),
            scratch_shapes=[
                wide, wide, pltpu.VMEM((n_rows, 128), F32), pltpu.VMEM((4, tok_count), F32),
                pltpu.VMEM((model_dim, ff_dim), BF16), pltpu.VMEM((model_dim, ff_dim), BF16),
                pltpu.VMEM((ff_dim, model_dim), BF16), wide, wide, wide, narrow, narrow, narrow,
                pltpu.VMEM((model_dim, ff_dim), F32), pltpu.VMEM((model_dim, ff_dim), F32),
                pltpu.VMEM((ff_dim, model_dim), F32),
                pltpu.SemaphoreType.DMA((4, 3)), pltpu.SemaphoreType.DMA((3,)),
                pltpu.SemaphoreType.DMA((4, 2)), pltpu.SemaphoreType.DMA((3,)),
            ],
            compiler_params=params(56), cost_estimate=cost(18 * n_rows * model_dim * ff_dim, 20e6), name="experts",
        )(*args)

    def combine(t, *args):
        tile = 256
        pick = pl.BlockSpec((1, capacity, model_dim), lambda i: (t, 0, 0))
        out = pl.BlockSpec((tile, model_dim), lambda i: (i, 0))
        return pl.pallas_call(
            functools.partial(combine_kernel, capacity), grid=(tok_count // tile,),
            out_shape=(shape((tok_count, model_dim), F32),) * 2,
            in_specs=[pick] * 16 + [small] * 2, out_specs=(out, out),
            compiler_params=params(dimension_semantics=("arbitrary",)),
            cost_estimate=cost(32 * capacity * tok_count * model_dim, 20e6), name="combine",
        )(*args)

    return gather, experts, combine


def solution(mesh):
    n_dev = mesh.shape["ep"]

    def block_body(x_loc, w_router, wg_loc, wu_loc, wd_loc, idx_loc, dy_loc):
        tok_count, model_dim = x_loc.shape
        top_k = idx_loc.shape[1]
        n_exp = w_router.shape[1]
        ff_dim = wg_loc.shape[2]
        capacity = (5 * tok_count * top_k + 4 * n_exp - 1) // (4 * n_exp)
        n_total = tok_count * n_dev
        vmem = pl.BlockSpec(memory_space=pltpu.VMEM)
        smem = pl.BlockSpec(memory_space=pltpu.SMEM)
        shape = jax.ShapeDtypeStruct
        me = lax.axis_index("ep")
        core = me % 2
        column = (me // 2) % 4
        ring_pos = jnp.array([0, 1, 3, 2], jnp.int32)[me // 8]
        ring_arr = jnp.array(RING, jnp.int32)

        def expert_ids(col):
            dist = jnp.arange(4, dtype=jnp.int32)
            z_of = ring_arr[(ring_pos - dist + 4) % 4]
            base = z_of * 8 + col * 2
            return jnp.stack([base + core, base + 1 - core], axis=1).reshape(8)

        eid = expert_ids(column)
        eid_all = jnp.concatenate([eid, expert_ids(column ^ 1), expert_ids(column ^ 2), expert_ids(column ^ 3)])
        idx_t = idx_loc.T

        x_x, dy_x = send(x_loc, PERM_X), send(dy_loc, PERM_X)
        x_y, dy_y = send(x_loc, PERM_Y), send(dy_loc, PERM_Y)
        x_d, dy_d = send(x_x, PERM_Y), send(dy_y, PERM_X)
        xs_all = (x_loc, x_x, x_y, x_d)
        dys_all = (dy_loc, dy_x, dy_y, dy_d)

        mine = [(wg_loc[0], wu_loc[0], wd_loc[0])]
        for _ in range(1, 4):
            mine.append(tuple(send(w, PERM_Z) for w in mine[-1]))
        other = [tuple(send(w, PERM_C) for w in ws) for ws in mine]

        prob, meta, stat = pl.pallas_call(
            functools.partial(route_kernel, capacity),
            out_shape=(shape((n_exp, tok_count), F32), shape((2 * n_exp, tok_count), F32), shape((n_exp, tok_count), F32)),
            in_specs=[vmem] * 3, out_specs=(vmem,) * 3, compiler_params=params(),
            cost_estimate=cost(4e9, 4e6), name="route",
        )(x_loc, w_router, idx_t)
        stat = lax.psum(stat, "ep")
        meta_x, meta_y = send(meta, PERM_X), send(meta, PERM_Y)
        meta_d = send(meta, PERM_D)
        load_frac = stat[:, 0:1] / (n_total * top_k)
        mean_prob = stat[:, tok_count - 1:] / n_total
        aux_loss = AUX_COEF * n_exp * jnp.sum(load_frac * mean_prob)

        gather, expert_call, combine_call = make_calls(capacity, tok_count, model_dim, ff_dim, n_exp)
        metas = (meta, meta_x, meta_y, meta_d)
        gathered = []
        for t in range(4):
            gathered.append(gather(eid, xs_all[t], dys_all[t], metas[t]))
        xs, dr, ws, pos, gate = zip(*gathered)

        o_j, dx_j, a_j = [None] * 8, [None] * 8, [None] * 8
        travel = None
        for k in (1, 2, 3, 0):
            j = 2 * k + 1
            o_j[j], dx_j[j], a_j[j], *dw_other = expert_call(j, *xs, *dr, *ws, *pos, *other[k])
            dw_sib = [send(part, PERM_C) for part in dw_other]
            j = 2 * k
            o_j[j], dx_j[j], a_j[j], *dw_mine = expert_call(j, *xs, *dr, *ws, *pos, *mine[k])
            total = [own + sib for own, sib in zip(dw_mine, dw_sib)]
            if travel is not None:
                total = [part + came for part, came in zip(total, travel)]
            travel = [send(part, PERM_Z) for part in total] if k else total
        dw_gate, dw_up, dw_down = (part[None] for part in travel)

        def combine(t):
            return combine_call(t, *o_j, *dx_j, pos[t], gate[t])

        y_d, dx_d = combine(3)
        y_d_in, dx_d_in = send(y_d, PERM_X), send(dx_d, PERM_Y)
        y_x, dx_x = combine(1)
        y_x_in = send(y_x, PERM_X)
        y_y, dx_y = combine(2)
        dx_y_in = send(dx_y, PERM_Y)
        y_y_in = send(y_y + y_d_in, PERM_Y)
        dx_x_in = send(dx_x + dx_d_in, PERM_X)
        y_0, dx_0 = combine(0)

        def a_rows(t):
            return jnp.concatenate([a_j[j][t:t + 1] for j in range(8)], axis=0)

        a_in = [a_rows(0), send(a_rows(1), PERM_X), send(a_rows(2), PERM_Y), send(a_rows(3), PERM_D)]
        dwr_t, dx_r = pl.pallas_call(
            functools.partial(router_kernel, AUX_COEF * n_exp / n_total),
            out_shape=(shape((n_exp, model_dim), F32), shape((tok_count, model_dim), F32)),
            in_specs=[smem] + [vmem] * 9, out_specs=(vmem,) * 2,
            scratch_shapes=[pltpu.VMEM((n_exp, tok_count), F32)],
            compiler_params=params(), cost_estimate=cost(1e9, 8e6), name="router",
        )(eid_all, *a_in, prob, idx_t, load_frac, w_router, x_loc)
        dw_router = lax.psum(dwr_t, "ep").T
        y_loc = (y_0 + y_x_in + y_y_in).astype(BF16)
        dx_loc = (dx_0 + dx_y_in + dx_x_in + dx_r).astype(BF16)
        return y_loc, aux_loss, dx_loc, dw_router, dw_gate, dw_up, dw_down

    tok_spec = P("ep")
    return jax.shard_map(
        block_body,
        mesh=mesh,
        in_specs=(tok_spec, P(), tok_spec, tok_spec, tok_spec, tok_spec, tok_spec),
        out_specs=(tok_spec, P(), tok_spec, P(), tok_spec, tok_spec, tok_spec),
        check_vma=False,
    )
```
